32 devices in a mesh: parts: 2 (over y), gz: 4 (over z), gy: 2 (over x), lc: 2 (over core).
Axes of the slice: x: 2, y: 2, z: 4, core: 2. Of those that a mesh axis runs over, the one named last changes fastest.
Arguments:
- density: float32 [64, 128, 256], P(('parts', 'gz'), 'gy'), parts along dimension 0, may hold values from 0.05 to 1
- void_mask: int32 [64, 128, 256], P(('parts', 'gz'), 'gy'), parts along dimension 0, may hold values 0 or 1
- fixed_mask: int32 [64, 128, 256], P(('parts', 'gz'), 'gy'), parts along dimension 0, may hold values 0 or 1
- displacement: float32 [2, 3, 64, 128, 256], P('lc', None, ('parts', 'gz'), 'gy'), parts along dimension 2, may hold values from -4 to 4
- load_ratio: int32 [4], P('parts'), parts along dimension 0, may hold values from 1 to 8
Outputs:
- gradient: float32 [64, 128, 256], P(('parts', 'gz'), 'gy'), parts along dimension 0
The draws below stay inside these ranges and needn't reach their ends.
There are 2 independent parts, one for each index of `parts`. The reference program is written for one: setup_inputs(seed, part) draws one part's arguments, and reference() takes and returns one part's arrays. A program takes and returns all parts, laid end to end along the dimension named above; each array names one. Nothing has to cross between parts.
All inputs are finite; a program needn't handle non-finite values. No bound on the sum of `void_mask` or of `fixed_mask` on one device may be relied on, other than what follows from the above.
Results may differ from the reference program's by a relative error of at most 0.0001.
Values sent between devices are 32-bit elements; how exact they have to be, the bound alone decides.
A program may use at most 64 MiB of HBM per device.

```python
import math
import jax
import jax.numpy as jnp
import numpy as np
from jax import lax

NZ = 256
NX = 32
NY = 128
LC = 2


def with_ends(values, rng, low, high):
    dims = values.shape
    spot = [jax.random.randint(jax.random.fold_in(rng, axis), (), 0, dims[axis]) for axis in range(len(dims))]
    values = values.at[tuple(spot)].set(low)
    longest = dims.index(max(dims))
    spot[longest] = (spot[longest] + 1) % dims[longest]
    return values.at[tuple(spot)].set(high)


def block_scale(key, extent, cuts, least, top_value):
    factor_of, own = 1.0, jax.random.fold_in(key, 6)
    for axis_at, shards_of in cuts:
        steps = jnp.exp(jax.random.uniform(jax.random.fold_in(own, axis_at), (shards_of,), jnp.float32, least / len(cuts), top_value / len(cuts)))
        factor_of = factor_of * jnp.repeat(steps, extent[axis_at] // shards_of).reshape([-1 if axis == axis_at else 1 for axis in range(len(extent))])
    return factor_of


def scatter_about(own_key, dims, deviation, bound, cuts=(), kind=jnp.bfloat16):
    gain = block_scale(own_key, dims, cuts, -0.22, 0.18) if cuts else 1.0
    entries = jax.random.normal(own_key, dims, jnp.float32) * deviation * gain
    return jnp.minimum(jnp.maximum(entries, -bound), bound).astype(kind)


def setup_inputs(seed: int = 0, part: int = 0) -> dict:
    key_list = jax.random.split(jax.random.key(seed), 6)
    part_keys = jax.random.split(jax.random.fold_in(key_list[5], part), 6)
    return {
        "density": jnp.clip(0.05 + 0.95 * jax.random.uniform(part_keys[0], (NX, NY, NZ), jnp.float32) ** block_scale(part_keys[0], (NX, NY, NZ), ((0, 4), (1, 2)), -0.2, 0.2), 0.05, 1.0),
        "void_mask": with_ends((jax.random.randint(part_keys[1], (NX, NY, NZ), 0, 8) < 1).astype(jnp.int32), jax.random.fold_in(part_keys[1], 1), 0, 1),
        "fixed_mask": with_ends((jax.random.randint(part_keys[2], (NX, NY, NZ), 0, 8) < 1).astype(jnp.int32), jax.random.fold_in(part_keys[2], 1), 0, 1),
        "displacement": scatter_about(part_keys[3], (LC, 3, NX, NY, NZ), 0.3, 4.0, ((0, 2), (2, 4), (3, 2)), jnp.float32),
        "load_ratio": jax.random.randint(part_keys[4], (LC,), 1, 9).astype(jnp.int32),
    }


def element_stiffness():
    poisson = 0.3
    factor = 1.0 / ((1.0 + poisson) * (1.0 - 2.0 * poisson))
    material = np.zeros((6, 6))
    material[:3, :3] = poisson
    for index in range(3):
        material[index, index] = 1.0 - poisson
        material[index + 3, index + 3] = 0.5 - poisson
    material = material * factor
    corners = [(first, second, third) for first in (0, 1) for second in (0, 1) for third in (0, 1)]
    points = [0.5 - 0.5 / math.sqrt(3.0), 0.5 + 0.5 / math.sqrt(3.0)]
    stiffness = np.zeros((24, 24))
    for point_x in points:
        for point_y in points:
            for point_z in points:
                strain = np.zeros((6, 24))
                for corner_index, (first, second, third) in enumerate(corners):
                    along_x = point_x if first else 1.0 - point_x
                    along_y = point_y if second else 1.0 - point_y
                    along_z = point_z if third else 1.0 - point_z
                    sign_x = 1.0 if first else -1.0
                    sign_y = 1.0 if second else -1.0
                    sign_z = 1.0 if third else -1.0
                    deriv_x = sign_x * along_y * along_z
                    deriv_y = along_x * sign_y * along_z
                    deriv_z = along_x * along_y * sign_z
                    column = 3 * corner_index
                    strain[0, column] = deriv_x
                    strain[1, column + 1] = deriv_y
                    strain[2, column + 2] = deriv_z
                    strain[3, column] = deriv_y
                    strain[3, column + 1] = deriv_x
                    strain[4, column + 1] = deriv_z
                    strain[4, column + 2] = deriv_y
                    strain[5, column] = deriv_z
                    strain[5, column + 2] = deriv_x
                stiffness = stiffness + 0.125 * strain.T @ material @ strain
    return stiffness

def cone_offsets():
    result = []
    for shift_x in range(-2, 3):
        for shift_y in range(-2, 3):
            for shift_z in range(-2, 3):
                dist_sq = shift_x * shift_x + shift_y * shift_y + shift_z * shift_z
                if dist_sq < 6.25:
                    result.append((shift_x, shift_y, shift_z, 2.5 - math.sqrt(dist_sq)))
    return result

def cone_filter(padded, shape):
    rows_x, rows_y, depth = shape
    total = jnp.zeros(shape, padded.dtype)
    for shift_x, shift_y, shift_z, weight in cone_offsets():
        total = total + weight * padded[2 + shift_x:2 + shift_x + rows_x, 2 + shift_y:2 + shift_y + rows_y, 2 + shift_z:2 + shift_z + depth]
    return total

def strain_energy(moved):
    rows_x, rows_y, depth = (moved.shape[1], moved.shape[2], moved.shape[3])
    extended = jnp.pad(moved, ((0, 0), (0, 1), (0, 1), (0, 1)))
    stiffness = jnp.asarray(element_stiffness(), moved.dtype)

    def one_layer(layer):
        layers = lax.dynamic_slice_in_dim(extended, layer, 2, 1)
        nodes = []
        for first in (0, 1):
            for second in (0, 1):
                for third in (0, 1):
                    nodes.append(layers[:, first, second:second + rows_y, third:third + depth])
        flat = jnp.stack(nodes, 0).reshape(24, rows_y * depth)
        product = jnp.dot(stiffness, flat, precision=lax.Precision.HIGHEST)
        return lax.optimization_barrier(jnp.sum(flat * product, 0)).reshape(rows_y, depth)
    return lax.map(one_layer, jnp.arange(rows_x, dtype=jnp.int32))

def reference(density, void_mask, fixed_mask, displacement, load_ratio):
    shape = density.shape
    weight_sum = cone_filter(jnp.pad(jnp.ones_like(density), 2), shape)
    physical = cone_filter(jnp.pad(density, 2), shape) / weight_sum
    free = (1 - fixed_mask).astype(density.dtype)
    ratios = load_ratio.astype(density.dtype)
    shares = ratios / jnp.sum(ratios)
    weighted = jnp.zeros(shape, density.dtype)
    for case in range(displacement.shape[0]):
        energy = strain_energy(displacement[case] * free[None])
        weighted = weighted + shares[case] * energy
    alive = (1 - void_mask).astype(density.dtype)
    sensed = alive * (-3.0 * physical * physical * (1.0 - 0.001)) * weighted / weight_sum
    return alive * cone_filter(jnp.pad(sensed, 2), shape)
```

```python
import math

import jax
import jax.numpy as jnp
from jax import lax
from jax.experimental import pallas as pl
from jax.experimental.pallas import tpu as pltpu
from jax.sharding import PartitionSpec as P

MESH = pl.DeviceIdType.MESH
POISSON = 0.3
FACTOR = 1.0 / ((1.0 + POISSON) * (1.0 - 2.0 * POISSON))
LAMBDA = POISSON * FACTOR
SHEAR = (0.5 - POISSON) * FACTOR
W = [2.5 - math.sqrt(d) for d in range(7)]
N_COPIES = 19


def layer_classes(q0, q1, q2, q4, q5):
    p0 = W[0] * q0 + W[1] * q1 + W[2] * q2 + W[4] * q4 + W[5] * q5
    p1 = W[1] * q0 + W[2] * q1 + W[3] * q2 + W[5] * q4 + W[6] * q5
    p2 = W[4] * q0 + W[5] * q1 + W[6] * q2
    return p0, p1, p2


def lane_index(shape):
    return lax.broadcasted_iota(jnp.int32, shape, len(shape) - 1)


def lane_pair(field, step):
    depth = field.shape[-1]
    lane = lane_index(field.shape)
    after = jnp.where(lane < depth - step, pltpu.roll(field, depth - step, 1), 0.0)
    before = jnp.where(lane >= step, pltpu.roll(field, step, 1), 0.0)
    return after + before


def cone_tile(ref, layer, row):
    f = [ref[layer + k, pl.ds(row, 24), :] for k in range(5)]
    x0, x1, x2 = f[2], f[1] + f[3], f[0] + f[4]

    def pair(t, step):
        return (pltpu.roll(t, step, 0) + pltpu.roll(t, 24 - step, 0))[8:16]

    q0 = x0[8:16]
    q1 = x1[8:16] + pair(x0, 1)
    q2 = pair(x1, 1)
    q4 = x2[8:16] + pair(x0, 2)
    q5 = pair(x2, 1) + pair(x1, 2)
    p0, p1, p2 = layer_classes(q0, q1, q2, q4, q5)
    return p0 + lane_pair(p1, 1) + lane_pair(p2, 2)


def present(position, total, step):
    before = (position >= step).astype(jnp.float32)
    return before + (position + step < total).astype(jnp.float32)


def weight_tile(layer, layers, row, rows, depth):
    shape = (8, depth)
    sub = lax.broadcasted_iota(jnp.int32, shape, 0) + row
    spot = jnp.full(shape, layer, jnp.int32)
    nx1, nx2 = present(spot, layers, 1), present(spot, layers, 2)
    ny1, ny2 = present(sub, rows, 1), present(sub, rows, 2)
    one = jnp.ones(shape, jnp.float32)
    p0, p1, p2 = layer_classes(one, nx1 + ny1, nx1 * ny1, nx2 + ny2, nx2 * ny1 + nx1 * ny2)
    lane = lane_index(shape)
    return p0 + present(lane, depth, 1) * p1 + present(lane, depth, 2) * p2


def node_modes(ref, comp, layer, row):
    t = ref[comp, layer, pl.ds(row, 16), :]
    depth = t.shape[-1]
    tn = jnp.where(lane_index(t.shape) < depth - 1, pltpu.roll(t, depth - 1, 1), 0.0)
    s, d = t + tn, tn - t
    s0, d0 = s[0:8], d[0:8]
    s1, d1 = pltpu.roll(s, 15, 0)[0:8], pltpu.roll(d, 15, 0)[0:8]
    return s0 + s1, d0 + d1, s1 - s0, d1 - d0


def energy_tile(ref, layer, row):
    modes = []
    for comp in range(3):
        a = node_modes(ref, comp, layer, row)
        b = node_modes(ref, comp, layer + 1, row)
        modes.append(
            {
                "x": b[0] - a[0],
                "z": a[1] + b[1],
                "y": a[2] + b[2],
                "yz": a[3] + b[3],
                "xz": b[1] - a[1],
                "xy": b[2] - a[2],
                "xyz": b[3] - a[3],
            }
        )
    u, v, w = modes
    sq = lambda t: t * t
    trace = sq(u["x"] + v["y"] + w["z"])
    linear = sq(v["xy"] + w["xz"]) + sq(u["xy"] + w["yz"]) + sq(u["xz"] + v["yz"])
    normal = sq(u["x"]) + sq(v["y"]) + sq(w["z"])
    bend = sq(u["xy"]) + sq(u["xz"]) + sq(v["xy"]) + sq(v["yz"]) + sq(w["yz"]) + sq(w["xz"])
    shear = sq(u["y"] + v["x"]) + sq(u["z"] + w["x"]) + sq(v["z"] + w["y"])
    twist = sq(u["yz"] + v["xz"]) + sq(u["yz"] + w["xy"]) + sq(v["xz"] + w["xy"])
    cubic = sq(u["xyz"]) + sq(v["xyz"]) + sq(w["xyz"])
    return (1.0 / 16.0) * (
        LAMBDA * trace
        + (LAMBDA / 3.0) * linear
        + (2.0 * SHEAR) * normal
        + SHEAR * (bend + shear)
        + (SHEAR / 3.0) * twist
        + ((LAMBDA + 4.0 * SHEAR) / 9.0) * cubic
    )


def kernel(
    ratio, density, void, fixed, disp, out,
    moved, fix, col_s, col_r, cor_s, cor_r, dens, dead, scale, energy, other, sens, grad,
    local, send, recv,
):
    layers, rows, depth = density.shape
    half = layers // 2
    tiles = rows // 8
    r, c, h = lax.axis_index("gz"), lax.axis_index("gy"), lax.axis_index("lc")
    nr, nc = lax.axis_size("gz"), lax.axis_size("gy")
    dz = 1 - 2 * h
    mid = pl.ds(8, rows)
    low, high = pl.ds(0, 8), pl.ds(rows + 8, 8)

    def there(step_z, step_y):
        z, y = r + step_z, c + step_y
        return (z >= 0) & (z < nr) & (y >= 0) & (y < nc)

    def remote(index, src, dst, step_z, step_y, core):
        copy = pltpu.make_async_remote_copy(
            src_ref=src, dst_ref=dst, send_sem=send.at[index], recv_sem=recv.at[index],
            device_id={"gz": r + step_z, "gy": c + step_y, "lc": core}, device_id_type=MESH,
        )
        goes, comes = there(step_z, step_y), there(-step_z, -step_y)
        return copy, goes, comes

    def start(entry):
        copy, goes, _ = entry
        pl.when(goes)(copy.start)

    def arrive(entry):
        copy, _, comes = entry
        pl.when(comes)(copy.wait_recv)

    def left(entry):
        copy, goes, _ = entry
        pl.when(goes)(copy.wait_send)

    l0, b0 = half // 2 * (1 - h), half // 2 * h
    keep = half + 2
    lz, sb = (half + 2) * h, (layers - 2) * (1 - h)
    get_disp = pltpu.make_async_copy(
        disp.at[0], moved.at[:, pl.ds(0, layers), pl.ds(0, rows), :], local.at[0]
    )
    get_fix = pltpu.make_async_copy(fixed, fix, local.at[1])
    get_dens = pltpu.make_async_copy(
        density.at[pl.ds(b0, keep)], dens.at[pl.ds(l0, keep), mid, :], local.at[2]
    )
    get_dead = pltpu.make_async_copy(void.at[pl.ds(half * h, half)], dead, local.at[3])
    for copy in (get_disp, get_fix, get_dens, get_dead):
        copy.start()

    barrier = pltpu.get_barrier_semaphore()
    for step_z in (-1, 0, 1):
        for step_y in (-1, 0, 1):
            for flip in (0, 1):
                if step_z == 0 and step_y == 0 and flip == 0:
                    continue
                core = h if flip == 0 else 1 - h

                @pl.when(there(step_z, step_y))
                def _():
                    pl.semaphore_signal(
                        barrier, inc=1,
                        device_id={"gz": r + step_z, "gy": c + step_y, "lc": core},
                        device_id_type=MESH,
                    )

    span_z = 1 + (r > 0).astype(jnp.int32) + (r < nr - 1).astype(jnp.int32)
    span_y = 1 + (c > 0).astype(jnp.int32) + (c < nc - 1).astype(jnp.int32)
    pl.semaphore_wait(barrier, 2 * span_z * span_y - 1)

    own, edge = pl.ds(b0, keep), pl.ds(sb, 2)
    top, bottom = pl.ds(rows - 8, 8), pl.ds(0, 8)
    near, far = pl.ds(l0, keep), pl.ds(lz, 2)
    dens_copies = [
        remote(0, density.at[edge], dens.at[far, mid, :], dz, 0, h),
        remote(1, density.at[own, top, :], dens.at[near, low, :], 0, 1, h),
        remote(2, density.at[own, bottom, :], dens.at[near, high, :], 0, -1, h),
        remote(3, density.at[edge, top, :], dens.at[far, low, :], dz, 1, h),
        remote(4, density.at[edge, bottom, :], dens.at[far, high, :], dz, -1, h),
    ]

    get_disp.wait()
    get_fix.wait()

    def free_layer(i, _):
        free = (1 - fix[i]).astype(jnp.float32)
        for comp in range(3):
            moved[comp, i, pl.ds(0, rows), :] = moved[comp, i, pl.ds(0, rows), :] * free
        return 0

    lax.fori_loop(0, layers, free_layer, 0)
    for comp in range(3):
        for i in range(layers):
            col_s[comp, i : i + 1, :] = moved[comp, i, 0:1, :]
        cor_s[comp : comp + 1, :] = moved[comp, 0, 0:1, :]
    plane = pl.ds(0, rows)
    send_layer = remote(
        5, moved.at[:, 0, plane, :], moved.at[:, layers, plane, :], -1, 0, h
    )
    send_col = remote(6, col_s, col_r, 0, -1, h)
    send_cor = remote(7, cor_s, cor_r, -1, -1, h)
    for entry in (send_col, send_cor, send_layer):
        start(entry)
    for entry in dens_copies:
        start(entry)

    @pl.when(r == nr - 1)
    def _():
        for comp in range(3):
            moved[comp, layers, plane, :] = jnp.zeros((rows, depth), jnp.float32)

    @pl.when(c == nc - 1)
    def _():
        col_r[...] = jnp.zeros_like(col_r)

    @pl.when(jnp.logical_not(there(1, 1)))
    def _():
        cor_r[...] = jnp.zeros_like(cor_r)

    blank = jnp.zeros((8, depth), jnp.float32)
    for ref in (dens, sens):

        @pl.when(c == 0)
        def _():
            for i in range(half + 4):
                ref[i, low, :] = blank

        @pl.when(c == nc - 1)
        def _():
            for i in range(half + 4):
                ref[i, high, :] = blank

        @pl.when(jnp.logical_not(there(-dz, 0)))
        def _():
            for i in range(2):
                ref[lz + i] = jnp.zeros((rows + 16, depth), jnp.float32)

    arrive(send_col)
    for comp in range(3):
        for i in range(layers):
            moved[comp, i, pl.ds(rows, 1), :] = col_r[comp, i : i + 1, :]

    ratio_sum = ratio[0]
    for case in range(1, ratio.shape[0]):
        ratio_sum = ratio_sum + ratio[case]
    share = jnp.full((8, depth), ratio[h].astype(jnp.float32)) / jnp.full(
        (8, depth), ratio_sum.astype(jnp.float32)
    )

    def energy_layer(i):
        def tile(j, _):
            row = pl.multiple_of(j * 8, 8)
            energy[i, pl.ds(row, 8), :] = share * energy_tile(moved, i, row)
            return 0

        lax.fori_loop(0, tiles, tile, 0)

    def energy_step(k, _):
        energy_layer(lax.rem(k + half * (1 - h), layers - 1))
        return 0

    give = half * (1 - h)
    swap_a = remote(
        8, energy.at[pl.ds(give, half - 1)], other.at[pl.ds(0, half - 1)], 0, 0, 1 - h
    )
    swap_b = remote(
        9, energy.at[pl.ds(give + half - 1, 1)], other.at[pl.ds(half - 1, 1)], 0, 0, 1 - h
    )
    lax.fori_loop(0, half - 1, energy_step, 0)
    start(swap_a)
    lax.fori_loop(half - 1, half, energy_step, 0)
    pl.when(h == 1)(swap_b[0].start)
    lax.fori_loop(half, layers - 1, energy_step, 0)

    get_dens.wait()
    get_dead.wait()
    for entry in dens_copies:
        arrive(entry)

    def scale_step(n, _):
        j, k = n // tiles, lax.rem(n, tiles)
        row = pl.multiple_of(k * 8, 8)
        weights = weight_tile(
            r * layers + half * h + j, nr * layers, c * rows + row, nc * rows, depth
        )
        inverse = 1.0 / weights
        physical = cone_tile(dens, j, row) * inverse
        alive = (1 - dead[j, pl.ds(row, 8), :]).astype(jnp.float32)
        scale[j, pl.ds(row, 8), :] = (
            alive * (-3.0 * (1.0 - 0.001)) * physical * physical * inverse
        )
        return 0

    lax.fori_loop(0, half * tiles, scale_step, 0)

    arrive(send_layer)
    arrive(send_cor)
    for comp in range(3):
        moved[comp, layers, pl.ds(rows, 1), :] = cor_r[comp : comp + 1, :]
    energy_layer(layers - 1)
    pl.when(h == 0)(swap_b[0].start)
    arrive(swap_a)
    arrive(swap_b)

    def sense_step(j, _):
        sens[2 + j, mid, :] = scale[j] * (energy[half * h + j] + other[j])
        return 0

    lax.fori_loop(0, half, sense_step, 0)
    ps, pd = pl.ds(half - (half - 2) * h, 2), pl.ds((half + 2) * h, 2)
    zs, zd = pl.ds(2 + (half - 2) * h, 2), pl.ds((half + 2) * (1 - h), 2)
    rest = pl.ds(2, half)
    last, first = pl.ds(rows, 8), pl.ds(8, 8)
    sense_copies = [
        remote(11, sens.at[zs, mid, :], sens.at[zd, mid, :], -dz, 0, 1 - h),
        remote(10, sens.at[ps, mid, :], sens.at[pd, mid, :], 0, 0, 1 - h),
        remote(16, sens.at[zs, last, :], sens.at[zd, low, :], -dz, 1, 1 - h),
        remote(17, sens.at[zs, first, :], sens.at[zd, high, :], -dz, -1, 1 - h),
        remote(12, sens.at[rest, last, :], sens.at[rest, low, :], 0, 1, h),
        remote(13, sens.at[rest, first, :], sens.at[rest, high, :], 0, -1, h),
        remote(14, sens.at[ps, last, :], sens.at[pd, low, :], 0, 1, 1 - h),
        remote(15, sens.at[ps, first, :], sens.at[pd, high, :], 0, -1, 1 - h),
    ]
    sides = {11: (-dz, 0), 16: (-dz, -1), 17: (-dz, 1)}
    numbers = (11, 10, 16, 17, 12, 13, 14, 15)
    sense_copies = [
        (copy, goes, there(*sides[n]) if n in sides else comes)
        for n, (copy, goes, comes) in zip(numbers, sense_copies)
    ]
    for entry in sense_copies:
        start(entry)
    for entry in sense_copies:
        arrive(entry)

    def filter_step(n, _):
        j, k = n // tiles, lax.rem(n, tiles)
        row = pl.multiple_of(k * 8, 8)
        alive = (1 - dead[j, pl.ds(row, 8), :]).astype(jnp.float32)
        grad[j, pl.ds(row, 8), :] = alive * cone_tile(sens, j, row)
        return 0

    lax.fori_loop(0, half * tiles, filter_step, 0)
    place = pl.ds(half * h, half)
    put = pltpu.make_async_copy(grad, out.at[place], local.at[4])
    give_out = remote(18, grad, out.at[place], 0, 0, 1 - h)
    start(give_out)
    put.start()
    for entry in [*dens_copies, send_layer, send_col, send_cor, swap_a, swap_b, *sense_copies]:
        left(entry)
    left(give_out)
    arrive(give_out)
    put.wait()


def shards(density, void_mask, fixed_mask, displacement, load_ratio):
    layers, rows, depth = density.shape
    half = layers // 2
    f32 = jnp.float32
    hbm = pl.BlockSpec(memory_space=pl.ANY)
    return pl.pallas_call(
        kernel,
        out_shape=jax.ShapeDtypeStruct(density.shape, f32),
        in_specs=[pl.BlockSpec(memory_space=pltpu.SMEM), hbm, hbm, hbm, hbm],
        out_specs=hbm,
        scratch_shapes=[
            pltpu.VMEM((3, layers + 1, rows + 8, depth), f32),
            pltpu.VMEM((layers, rows, depth), jnp.int32),
            pltpu.VMEM((3, layers, depth), f32),
            pltpu.VMEM((3, layers, depth), f32),
            pltpu.VMEM((8, depth), f32),
            pltpu.VMEM((8, depth), f32),
            pltpu.VMEM((half + 4, rows + 16, depth), f32),
            pltpu.VMEM((half, rows, depth), jnp.int32),
            pltpu.VMEM((half, rows, depth), f32),
            pltpu.VMEM((layers, rows, depth), f32),
            pltpu.VMEM((half, rows, depth), f32),
            pltpu.VMEM((half + 4, rows + 16, depth), f32),
            pltpu.VMEM((half, rows, depth), f32),
            pltpu.SemaphoreType.DMA((5,)),
            pltpu.SemaphoreType.DMA((N_COPIES,)),
            pltpu.SemaphoreType.DMA((N_COPIES,)),
        ],
        compiler_params=pltpu.CompilerParams(collective_id=0, has_side_effects=True),
    )(load_ratio, density, void_mask, fixed_mask, displacement)


def solution(mesh):
    placed = (
        P(("parts", "gz"), "gy", None),
        P(("parts", "gz"), "gy", None),
        P(("parts", "gz"), "gy", None),
        P("lc", None, ("parts", "gz"), "gy", None),
        P("parts"),
    )
    return jax.shard_map(
        shards,
        mesh=mesh,
        in_specs=placed,
        out_specs=P(("parts", "gz"), "gy", None),
        check_vma=False,
    )
```

```python
import math

import jax
import jax.numpy as jnp
from jax import lax
from jax.experimental import pallas as pl
from jax.experimental.pallas import tpu as pltpu
from jax.sharding import PartitionSpec as P

MESH = pl.DeviceIdType.MESH
POISSON = 0.3
FACTOR = 1.0 / ((1.0 + POISSON) * (1.0 - 2.0 * POISSON))
LAMBDA = POISSON * FACTOR
SHEAR = (0.5 - POISSON) * FACTOR
W = [2.5 - math.sqrt(d) for d in range(7)]
N_COPIES = 24
TALL = 16
SHORT = 8


def layer_classes(q0, q1, q2, q4, q5):
    p0 = W[0] * q0 + W[1] * q1 + W[2] * q2 + W[4] * q4 + W[5] * q5
    p1 = W[1] * q0 + W[2] * q1 + W[3] * q2 + W[5] * q4 + W[6] * q5
    p2 = W[4] * q0 + W[5] * q1 + W[6] * q2
    return p0, p1, p2


def lane_index(shape):
    return lax.broadcasted_iota(jnp.int32, shape, len(shape) - 1)


def lane_pair(field, step):
    depth = field.shape[-1]
    lane = lane_index(field.shape)
    after = jnp.where(lane < depth - step, pltpu.roll(field, depth - step, 1), 0.0)
    before = jnp.where(lane >= step, pltpu.roll(field, step, 1), 0.0)
    return after + before


def cone_tiles(ref, layer, row, count):
    window = TALL + 16
    f = [ref[layer + k, pl.ds(row, window), :] for k in range(count + 4)]
    mid = slice(8, 8 + TALL)

    def pair(t, step):
        return (pltpu.roll(t, step, 0) + pltpu.roll(t, window - step, 0))[mid]

    result = []
    for k in range(count):
        x0, x1, x2 = f[k + 2], f[k + 1] + f[k + 3], f[k] + f[k + 4]
        q0 = x0[mid]
        q1 = x1[mid] + pair(x0, 1)
        q2 = pair(x1, 1)
        q4 = x2[mid] + pair(x0, 2)
        q5 = pair(x2, 1) + pair(x1, 2)
        p0, p1, p2 = layer_classes(q0, q1, q2, q4, q5)
        result.append(p0 + lane_pair(p1, 1) + lane_pair(p2, 2))
    return result


def present(position, total, step):
    before = (position >= step).astype(jnp.float32)
    return before + (position + step < total).astype(jnp.float32)


def weight_tile(layer, layers, row, rows, depth):
    shape = (TALL, depth)
    sub = lax.broadcasted_iota(jnp.int32, shape, 0) + row
    spot = jnp.full(shape, layer, jnp.int32)
    nx1, nx2 = present(spot, layers, 1), present(spot, layers, 2)
    ny1, ny2 = present(sub, rows, 1), present(sub, rows, 2)
    one = jnp.ones(shape, jnp.float32)
    p0, p1, p2 = layer_classes(one, nx1 + ny1, nx1 * ny1, nx2 + ny2, nx2 * ny1 + nx1 * ny2)
    lane = lane_index(shape)
    return p0 + present(lane, depth, 1) * p1 + present(lane, depth, 2) * p2


def node_modes(ref, layer, row):
    result = []
    for comp in range(3):
        t = ref[comp, layer, pl.ds(row, SHORT + 8), :]
        depth, window = t.shape[-1], t.shape[0]
        tn = jnp.where(lane_index(t.shape) < depth - 1, pltpu.roll(t, depth - 1, 1), 0.0)
        s, d = t + tn, tn - t
        s0, d0 = s[0:SHORT], d[0:SHORT]
        s1, d1 = pltpu.roll(s, window - 1, 0)[0:SHORT], pltpu.roll(d, window - 1, 0)[0:SHORT]
        result.append((s0 + s1, d0 + d1, s1 - s0, d1 - d0))
    return result


def energy_tile(lower, upper):
    modes = []
    for a, b in zip(lower, upper):
        modes.append(
            {
                "x": b[0] - a[0],
                "z": a[1] + b[1],
                "y": a[2] + b[2],
                "yz": a[3] + b[3],
                "xz": b[1] - a[1],
                "xy": b[2] - a[2],
                "xyz": b[3] - a[3],
            }
        )
    u, v, w = modes
    sq = lambda t: t * t
    trace = sq(u["x"] + v["y"] + w["z"])
    linear = sq(v["xy"] + w["xz"]) + sq(u["xy"] + w["yz"]) + sq(u["xz"] + v["yz"])
    normal = sq(u["x"]) + sq(v["y"]) + sq(w["z"])
    bend = sq(u["xy"]) + sq(u["xz"]) + sq(v["xy"]) + sq(v["yz"]) + sq(w["yz"]) + sq(w["xz"])
    shear = sq(u["y"] + v["x"]) + sq(u["z"] + w["x"]) + sq(v["z"] + w["y"])
    twist = sq(u["yz"] + v["xz"]) + sq(u["yz"] + w["xy"]) + sq(v["xz"] + w["xy"])
    cubic = sq(u["xyz"]) + sq(v["xyz"]) + sq(w["xyz"])
    return (1.0 / 16.0) * (
        LAMBDA * trace
        + (LAMBDA / 3.0) * linear
        + (2.0 * SHEAR) * normal
        + SHEAR * (bend + shear)
        + (SHEAR / 3.0) * twist
        + ((LAMBDA + 4.0 * SHEAR) / 9.0) * cubic
    )


def kernel(
    ratio, density, void, fixed, disp, out,
    moved, fix, col_s, col_r, cor_s, cor_r, dens, dead, scale, energy, other, sens,
    local, send, recv,
):
    layers, rows, depth = density.shape
    half = layers // 2
    r, c, h = lax.axis_index("gz"), lax.axis_index("gy"), lax.axis_index("lc")
    nr, nc = lax.axis_size("gz"), lax.axis_size("gy")
    dz = 1 - 2 * h
    mid = pl.ds(8, rows)
    low, high = pl.ds(0, 8), pl.ds(rows + 8, 8)

    def there(step_z, step_y):
        z, y = r + step_z, c + step_y
        return (z >= 0) & (z < nr) & (y >= 0) & (y < nc)

    def remote(index, src, dst, step_z, step_y, core):
        copy = pltpu.make_async_remote_copy(
            src_ref=src, dst_ref=dst, send_sem=send.at[index], recv_sem=recv.at[index],
            device_id={"gz": r + step_z, "gy": c + step_y, "lc": core}, device_id_type=MESH,
        )
        goes, comes = there(step_z, step_y), there(-step_z, -step_y)
        return copy, goes, comes

    def start(entry):
        copy, goes, _ = entry
        pl.when(goes)(copy.start)

    def arrive(entry):
        copy, _, comes = entry
        pl.when(comes)(copy.wait_recv)

    def left(entry):
        copy, goes, _ = entry
        pl.when(goes)(copy.wait_send)

    l0, b0 = half // 2 * (1 - h), half // 2 * h
    keep = half + 2
    lz, sb = (half + 2) * h, (layers - 2) * (1 - h)
    plane, others = pl.ds(0, rows), pl.ds(1, layers - 1)
    get_disp0 = pltpu.make_async_copy(disp.at[0, :, 0], moved.at[:, 0, plane, :], local.at[0])
    get_fix0 = pltpu.make_async_copy(fixed.at[0], fix.at[0], local.at[1])
    get_disp = pltpu.make_async_copy(
        disp.at[0, :, others], moved.at[:, others, plane, :], local.at[2]
    )
    get_fix = pltpu.make_async_copy(fixed.at[others], fix.at[others], local.at[3])
    get_dens = pltpu.make_async_copy(
        density.at[pl.ds(b0, keep)], dens.at[pl.ds(l0, keep), mid, :], local.at[4]
    )
    get_dead = pltpu.make_async_copy(void.at[pl.ds(half * h, half)], dead, local.at[5])
    for copy in (get_disp0, get_fix0, get_disp, get_fix, get_dens, get_dead):
        copy.start()

    barrier = pltpu.get_barrier_semaphore()
    for step_z in (-1, 0, 1):
        for step_y in (-1, 0, 1):
            for flip in (0, 1):
                if step_z == 0 and step_y == 0 and flip == 0:
                    continue
                core = h if flip == 0 else 1 - h

                @pl.when(there(step_z, step_y))
                def _():
                    pl.semaphore_signal(
                        barrier, inc=1,
                        device_id={"gz": r + step_z, "gy": c + step_y, "lc": core},
                        device_id_type=MESH,
                    )

    span_z = 1 + (r > 0).astype(jnp.int32) + (r < nr - 1).astype(jnp.int32)
    span_y = 1 + (c > 0).astype(jnp.int32) + (c < nc - 1).astype(jnp.int32)

    own, edge = pl.ds(b0, keep), pl.ds(sb, 2)
    top, bottom = pl.ds(rows - 8, 8), pl.ds(0, 8)
    near, far = pl.ds(l0, keep), pl.ds(lz, 2)
    dens_copies = [
        remote(0, density.at[edge], dens.at[far, mid, :], dz, 0, h),
        remote(1, density.at[own, top, :], dens.at[near, low, :], 0, 1, h),
        remote(2, density.at[own, bottom, :], dens.at[near, high, :], 0, -1, h),
        remote(3, density.at[edge, top, :], dens.at[far, low, :], dz, 1, h),
        remote(4, density.at[edge, bottom, :], dens.at[far, high, :], dz, -1, h),
    ]

    def free_layer(i, _):
        free = (1 - fix[i]).astype(jnp.float32)
        for comp in range(3):
            moved[comp, i, plane, :] = moved[comp, i, plane, :] * free
        return 0

    send_layer = remote(
        5, moved.at[:, 0, plane, :], moved.at[:, layers, plane, :], -1, 0, h
    )
    send_col = remote(6, col_s, col_r, 0, -1, h)
    send_cor = remote(7, cor_s, cor_r, -1, -1, h)
    get_disp0.wait()
    get_fix0.wait()
    free_layer(0, 0)
    for comp in range(3):
        cor_s[comp : comp + 1, :] = moved[comp, 0, 0:1, :]
    pl.semaphore_wait(barrier, 2 * span_z * span_y - 1)
    start(send_layer)
    start(send_cor)
    get_disp.wait()
    get_fix.wait()
    lax.fori_loop(1, layers, free_layer, 0)
    for comp in range(3):
        for i in range(layers):
            col_s[comp, i : i + 1, :] = moved[comp, i, 0:1, :]
    start(send_col)
    for entry in dens_copies:
        start(entry)

    @pl.when(r == nr - 1)
    def _():
        for comp in range(3):
            moved[comp, layers, plane, :] = jnp.zeros((rows, depth), jnp.float32)

    @pl.when(c == nc - 1)
    def _():
        col_r[...] = jnp.zeros_like(col_r)

    @pl.when(jnp.logical_not(there(1, 1)))
    def _():
        cor_r[...] = jnp.zeros_like(cor_r)

    blank = jnp.zeros((8, depth), jnp.float32)
    for ref in (dens, sens):

        @pl.when(c == 0)
        def _():
            for i in range(half + 4):
                ref[i, low, :] = blank

        @pl.when(c == nc - 1)
        def _():
            for i in range(half + 4):
                ref[i, high, :] = blank

        @pl.when(jnp.logical_not(there(-dz, 0)))
        def _():
            for i in range(2):
                ref[lz + i] = jnp.zeros((rows + 16, depth), jnp.float32)

    arrive(send_col)
    for comp in range(3):
        for i in range(layers):
            moved[comp, i, pl.ds(rows, 1), :] = col_r[comp, i : i + 1, :]

    ratio_sum = ratio[0]
    for case in range(1, ratio.shape[0]):
        ratio_sum = ratio_sum + ratio[case]
    share = jnp.full((8, depth), ratio[h].astype(jnp.float32)) / jnp.full(
        (8, depth), ratio_sum.astype(jnp.float32)
    )

    def energy_layers(first, count):
        def tile(j, _):
            row = pl.multiple_of(j * SHORT, SHORT)
            lower = node_modes(moved, first, row)
            for k in range(count):
                upper = node_modes(moved, first + k + 1, row)
                energy[first + k, pl.ds(row, SHORT), :] = share * energy_tile(lower, upper)
                lower = upper
            return 0

        lax.fori_loop(0, rows // SHORT, tile, 0)

    give = half * (1 - h)
    swap_a = remote(
        8, energy.at[pl.ds(give, half - 1)], other.at[pl.ds(0, half - 1)], 0, 0, 1 - h
    )
    swap_b = remote(
        9, energy.at[pl.ds(give + half - 1, 1)], other.at[pl.ds(half - 1, 1)], 0, 0, 1 - h
    )
    energy_layers(give, half - 1)
    start(swap_a)
    energy_layers((half - 1) * h, half)
    pl.when(h == 1)(swap_b[0].start)

    close, wide = 2 * (1 - h), 2 * h

    def scale_two(j):
        def tile(k, _):
            row = pl.multiple_of(k * TALL, TALL)
            cones = cone_tiles(dens, j, row, 2)
            for n in range(2):
                weights = weight_tile(
                    r * layers + half * h + j + n, nr * layers, c * rows + row, nc * rows, depth
                )
                inverse = 1.0 / weights
                physical = cones[n] * inverse
                alive = (1 - dead[j + n, pl.ds(row, TALL), :]).astype(jnp.float32)
                scale[j + n, pl.ds(row, TALL), :] = (
                    alive * (-3.0 * (1.0 - 0.001)) * physical * physical * inverse
                )
            return 0

        lax.fori_loop(0, rows // TALL, tile, 0)

    def sense_two(j):
        for n in range(2):
            sens[2 + j + n, mid, :] = scale[j + n] * (energy[half * h + j + n] + other[j + n])

    get_dens.wait()
    get_dead.wait()
    arrive(dens_copies[1])
    arrive(dens_copies[2])
    scale_two(close)
    arrive(swap_a)
    pl.when(h == 0)(swap_b[0].wait_recv)
    sense_two(close)

    ps, pd = pl.ds(half - (half - 2) * h, 2), pl.ds((half + 2) * h, 2)
    zs, zd = pl.ds(2 + (half - 2) * h, 2), pl.ds((half + 2) * (1 - h), 2)
    last, first = pl.ds(rows, 8), pl.ds(8, 8)
    close_copies = [
        remote(10, sens.at[ps, mid, :], sens.at[pd, mid, :], 0, 0, 1 - h),
        remote(12, sens.at[ps, last, :], sens.at[ps, low, :], 0, 1, h),
        remote(13, sens.at[ps, first, :], sens.at[ps, high, :], 0, -1, h),
        remote(14, sens.at[ps, last, :], sens.at[pd, low, :], 0, 1, 1 - h),
        remote(15, sens.at[ps, first, :], sens.at[pd, high, :], 0, -1, 1 - h),
    ]
    for entry in close_copies:
        start(entry)

    arrive(send_layer)
    arrive(send_cor)
    for comp in range(3):
        moved[comp, layers, pl.ds(rows, 1), :] = cor_r[comp : comp + 1, :]
    energy_layers(layers - 1, 1)
    pl.when(h == 0)(swap_b[0].start)
    for n in (0, 3, 4):
        arrive(dens_copies[n])
    scale_two(wide)
    pl.when(h == 1)(swap_b[0].wait_recv)
    sense_two(wide)

    def flipped(index, src, dst, step_y):
        copy, goes, _ = remote(index, src, dst, -dz, step_y, 1 - h)
        return copy, goes, there(-dz, -step_y)

    wide_copies = [
        flipped(11, sens.at[zs, mid, :], sens.at[zd, mid, :], 0),
        flipped(16, sens.at[zs, last, :], sens.at[zd, low, :], 1),
        flipped(17, sens.at[zs, first, :], sens.at[zd, high, :], -1),
    ]
    row_copies = [
        remote(18, sens.at[zs, last, :], sens.at[zs, low, :], 0, 1, h),
        remote(19, sens.at[zs, first, :], sens.at[zs, high, :], 0, -1, h),
    ]
    for entry in wide_copies + row_copies:
        start(entry)

    def filter_two(j):
        def tile(k, _):
            row = pl.multiple_of(k * TALL, TALL)
            cones = cone_tiles(sens, j, row, 2)
            for n in range(2):
                alive = (1 - dead[j + n, pl.ds(row, TALL), :]).astype(jnp.float32)
                out[half * h + j + n, pl.ds(row, TALL), :] = alive * cones[n]
            return 0

        lax.fori_loop(0, rows // TALL, tile, 0)

    def hand_over(index, j):
        place = pl.ds(half * h + j, 2)
        return remote(index, out.at[place], out.at[place], 0, 0, 1 - h)

    for entry in close_copies + row_copies:
        arrive(entry)
    filter_two(close)
    give_close, give_wide = hand_over(20, close), hand_over(21, wide)
    start(give_close)
    for entry in wide_copies:
        arrive(entry)
    filter_two(wide)
    start(give_wide)
    sent = [*dens_copies, send_layer, send_col, send_cor, swap_a, swap_b]
    for entry in sent + close_copies + wide_copies + row_copies + [give_close, give_wide]:
        left(entry)
    arrive(give_close)
    arrive(give_wide)


def shards(density, void_mask, fixed_mask, displacement, load_ratio):
    layers, rows, depth = density.shape
    half = layers // 2
    f32 = jnp.float32
    hbm = pl.BlockSpec(memory_space=pl.ANY)
    return pl.pallas_call(
        kernel,
        out_shape=pltpu.VMEM(density.shape, f32),
        in_specs=[pl.BlockSpec(memory_space=pltpu.SMEM), hbm, hbm, hbm, hbm],
        out_specs=pl.BlockSpec(memory_space=pltpu.VMEM),
        scratch_shapes=[
            pltpu.VMEM((3, layers + 1, rows + 8, depth), f32),
            pltpu.VMEM((layers, rows, depth), jnp.int32),
            pltpu.VMEM((3, layers, depth), f32),
            pltpu.VMEM((3, layers, depth), f32),
            pltpu.VMEM((8, depth), f32),
            pltpu.VMEM((8, depth), f32),
            pltpu.VMEM((half + 4, rows + 16, depth), f32),
            pltpu.VMEM((half, rows, depth), jnp.int32),
            pltpu.VMEM((half, rows, depth), f32),
            pltpu.VMEM((layers, rows, depth), f32),
            pltpu.VMEM((half, rows, depth), f32),
            pltpu.VMEM((half + 4, rows + 16, depth), f32),
            pltpu.SemaphoreType.DMA((6,)),
            pltpu.SemaphoreType.DMA((N_COPIES,)),
            pltpu.SemaphoreType.DMA((N_COPIES,)),
        ],
        compiler_params=pltpu.CompilerParams(collective_id=0, has_side_effects=True),
    )(load_ratio, density, void_mask, fixed_mask, displacement)


def solution(mesh):
    placed = (
        P(("parts", "gz"), "gy", None),
        P(("parts", "gz"), "gy", None),
        P(("parts", "gz"), "gy", None),
        P("lc", None, ("parts", "gz"), "gy", None),
        P("parts"),
    )
    return jax.shard_map(
        shards,
        mesh=mesh,
        in_specs=placed,
        out_specs=P(("parts", "gz"), "gy", None),
        check_vma=False,
    )
```

```python
import math

import jax
import jax.numpy as jnp
from jax import lax
from jax.experimental import pallas as pl
from jax.experimental.pallas import tpu as pltpu
from jax.sharding import PartitionSpec as P

MESH = pl.DeviceIdType.MESH
POISSON = 0.3
FACTOR = 1.0 / ((1.0 + POISSON) * (1.0 - 2.0 * POISSON))
LAMBDA = POISSON * FACTOR
SHEAR = (0.5 - POISSON) * FACTOR
W = [2.5 - math.sqrt(d) for d in range(7)]
N_COPIES = 40
CHUNKS = 4
TALL = 32
SHORT = 8


def layer_classes(q0, q1, q2, q4, q5):
    p0 = W[0] * q0 + W[1] * q1 + W[2] * q2 + W[4] * q4 + W[5] * q5
    p1 = W[1] * q0 + W[2] * q1 + W[3] * q2 + W[5] * q4 + W[6] * q5
    p2 = W[4] * q0 + W[5] * q1 + W[6] * q2
    return p0, p1, p2


def lane_index(shape):
    return lax.broadcasted_iota(jnp.int32, shape, len(shape) - 1)


def lane_pair(field, step):
    depth = field.shape[-1]
    lane = lane_index(field.shape)
    after = jnp.where(lane < depth - step, pltpu.roll(field, depth - step, 1), 0.0)
    before = jnp.where(lane >= step, pltpu.roll(field, step, 1), 0.0)
    return after + before


def cone_tiles(ref, layer, row, count):
    window = TALL + 16
    f = [ref[layer + k, pl.ds(row, window), :] for k in range(count + 4)]
    mid = slice(8, 8 + TALL)

    def pair(t, step):
        return (pltpu.roll(t, step, 0) + pltpu.roll(t, window - step, 0))[mid]

    result = []
    for k in range(count):
        x0, x1, x2 = f[k + 2], f[k + 1] + f[k + 3], f[k] + f[k + 4]
        q0 = x0[mid]
        q1 = x1[mid] + pair(x0, 1)
        q2 = pair(x1, 1)
        q4 = x2[mid] + pair(x0, 2)
        q5 = pair(x2, 1) + pair(x1, 2)
        p0, p1, p2 = layer_classes(q0, q1, q2, q4, q5)
        result.append(p0 + lane_pair(p1, 1) + lane_pair(p2, 2))
    return result


def present(position, total, step):
    before = (position >= step).astype(jnp.float32)
    return before + (position + step < total).astype(jnp.float32)


def weight_tile(layer, layers, row, rows, depth):
    shape = (TALL, depth)
    sub = lax.broadcasted_iota(jnp.int32, shape, 0) + row
    spot = jnp.full(shape, layer, jnp.int32)
    nx1, nx2 = present(spot, layers, 1), present(spot, layers, 2)
    ny1, ny2 = present(sub, rows, 1), present(sub, rows, 2)
    one = jnp.ones(shape, jnp.float32)
    p0, p1, p2 = layer_classes(one, nx1 + ny1, nx1 * ny1, nx2 + ny2, nx2 * ny1 + nx1 * ny2)
    lane = lane_index(shape)
    return p0 + present(lane, depth, 1) * p1 + present(lane, depth, 2) * p2


def node_modes(ref, layer, row):
    result = []
    for comp in range(3):
        t = ref[comp, layer, pl.ds(row, SHORT + 8), :]
        depth, window = t.shape[-1], t.shape[0]
        tn = jnp.where(lane_index(t.shape) < depth - 1, pltpu.roll(t, depth - 1, 1), 0.0)
        s, d = t + tn, tn - t
        s0, d0 = s[0:SHORT], d[0:SHORT]
        s1, d1 = pltpu.roll(s, window - 1, 0)[0:SHORT], pltpu.roll(d, window - 1, 0)[0:SHORT]
        result.append((s0 + s1, d0 + d1, s1 - s0, d1 - d0))
    return result


def energy_tile(lower, upper):
    modes = []
    for a, b in zip(lower, upper):
        modes.append(
            {
                "x": b[0] - a[0],
                "z": a[1] + b[1],
                "y": a[2] + b[2],
                "yz": a[3] + b[3],
                "xz": b[1] - a[1],
                "xy": b[2] - a[2],
                "xyz": b[3] - a[3],
            }
        )
    u, v, w = modes
    sq = lambda t: t * t
    trace = sq(u["x"] + v["y"] + w["z"])
    linear = sq(v["xy"] + w["xz"]) + sq(u["xy"] + w["yz"]) + sq(u["xz"] + v["yz"])
    normal = sq(u["x"]) + sq(v["y"]) + sq(w["z"])
    bend = sq(u["xy"]) + sq(u["xz"]) + sq(v["xy"]) + sq(v["yz"]) + sq(w["yz"]) + sq(w["xz"])
    shear = sq(u["y"] + v["x"]) + sq(u["z"] + w["x"]) + sq(v["z"] + w["y"])
    twist = sq(u["yz"] + v["xz"]) + sq(u["yz"] + w["xy"]) + sq(v["xz"] + w["xy"])
    cubic = sq(u["xyz"]) + sq(v["xyz"]) + sq(w["xyz"])
    return (1.0 / 16.0) * (
        LAMBDA * trace
        + (LAMBDA / 3.0) * linear
        + (2.0 * SHEAR) * normal
        + SHEAR * (bend + shear)
        + (SHEAR / 3.0) * twist
        + ((LAMBDA + 4.0 * SHEAR) / 9.0) * cubic
    )


def kernel(
    ratio, density, void, fixed, disp, out,
    moved, extra, fix, col_s, col_r, cor_s, cor_r, cor_x, dens, dead, scale, energy, other, sens,
    local, send, recv,
):
    layers, rows, depth = density.shape
    half = layers // 2
    r, c, h = lax.axis_index("gz"), lax.axis_index("gy"), lax.axis_index("lc")
    nr, nc = lax.axis_size("gz"), lax.axis_size("gy")
    dz = 1 - 2 * h
    mid = pl.ds(8, rows)
    low, high = pl.ds(0, 8), pl.ds(rows + 8, 8)

    def there(step_z, step_y):
        z, y = r + step_z, c + step_y
        return (z >= 0) & (z < nr) & (y >= 0) & (y < nc)

    def remote(index, src, dst, step_z, step_y, core):
        copy = pltpu.make_async_remote_copy(
            src_ref=src, dst_ref=dst, send_sem=send.at[index], recv_sem=recv.at[index],
            device_id={"gz": r + step_z, "gy": c + step_y, "lc": core}, device_id_type=MESH,
        )
        goes, comes = there(step_z, step_y), there(-step_z, -step_y)
        return copy, goes, comes

    def between(index, src, dst, step_z, step_y, giver, taker):
        copy, goes, comes = remote(index, src, dst, step_z, step_y, taker)
        return copy, goes & (h == giver), comes & (h == taker)

    def start(entry):
        copy, goes, _ = entry
        pl.when(goes)(copy.start)

    def arrive(entry):
        copy, _, comes = entry
        pl.when(comes)(copy.wait_recv)

    def left(entry):
        copy, goes, _ = entry
        pl.when(goes)(copy.wait_send)

    l0, b0 = half // 2 * (1 - h), half // 2 * h
    keep = half + 2
    lz, sb = (half + 2) * h, (layers - 2) * (1 - h)
    plane, others = pl.ds(0, rows), pl.ds(1, layers - 1)
    get_disp0 = pltpu.make_async_copy(disp.at[0, :, 0], moved.at[:, 0, plane, :], local.at[0])
    get_fix0 = pltpu.make_async_copy(fixed.at[0], fix.at[0], local.at[1])
    get_disp = pltpu.make_async_copy(
        disp.at[0, :, others], moved.at[:, others, plane, :], local.at[2]
    )
    get_fix = pltpu.make_async_copy(fixed.at[others], fix.at[others], local.at[3])
    get_dens = pltpu.make_async_copy(
        density.at[pl.ds(b0, keep)], dens.at[pl.ds(l0, keep), mid, :], local.at[4]
    )
    get_dead = pltpu.make_async_copy(void.at[pl.ds(half * h, half)], dead, local.at[5])
    for copy in (get_disp0, get_fix0, get_disp, get_fix, get_dens, get_dead):
        copy.start()

    barrier = pltpu.get_barrier_semaphore()
    for step_z in (-1, 0, 1):
        for step_y in (-1, 0, 1):
            for flip in (0, 1):
                if step_z == 0 and step_y == 0 and flip == 0:
                    continue
                core = h if flip == 0 else 1 - h

                @pl.when(there(step_z, step_y))
                def _():
                    pl.semaphore_signal(
                        barrier, inc=1,
                        device_id={"gz": r + step_z, "gy": c + step_y, "lc": core},
                        device_id_type=MESH,
                    )

    span_z = 1 + (r > 0).astype(jnp.int32) + (r < nr - 1).astype(jnp.int32)
    span_y = 1 + (c > 0).astype(jnp.int32) + (c < nc - 1).astype(jnp.int32)

    own, edge = pl.ds(b0, keep), pl.ds(sb, 2)
    top, bottom = pl.ds(rows - 8, 8), pl.ds(0, 8)
    near, far = pl.ds(l0, keep), pl.ds(lz, 2)
    dens_copies = [
        remote(0, density.at[edge], dens.at[far, mid, :], dz, 0, h),
        remote(1, density.at[own, top, :], dens.at[near, low, :], 0, 1, h),
        remote(2, density.at[own, bottom, :], dens.at[near, high, :], 0, -1, h),
        remote(3, density.at[edge, top, :], dens.at[far, low, :], dz, 1, h),
        remote(4, density.at[edge, bottom, :], dens.at[far, high, :], dz, -1, h),
    ]

    def free_layer(i, _):
        free = (1 - fix[i]).astype(jnp.float32)
        for comp in range(3):
            moved[comp, i, plane, :] = moved[comp, i, plane, :] * free
        return 0

    tall = rows // CHUNKS
    chunks = [pl.ds(q * tall, tall) for q in range(CHUNKS)]
    first_layer = [
        [
            between(24 + q, moved.at[:, 0, part, :], extra.at[:, 1, part, :], -1, 0, 0, 1),
            between(28 + q, moved.at[:, 0, part, :], moved.at[:, layers, part, :], -1, 0, 1, 1),
        ]
        for q, part in enumerate(chunks)
    ]
    send_col = remote(6, col_s, col_r, 0, -1, h)
    send_cor = [
        between(7, cor_s, cor_r, -1, -1, 1, 1),
        between(5, cor_s, cor_x, -1, -1, 0, 1),
    ]
    get_disp0.wait()
    get_fix0.wait()
    free_layer(0, 0)
    for comp in range(3):
        cor_s[comp : comp + 1, :] = moved[comp, 0, 0:1, :]
    pl.semaphore_wait(barrier, 2 * span_z * span_y - 1)
    for entry in [*send_cor, *first_layer[-1], dens_copies[0]]:
        start(entry)
    for pieces in first_layer[-2::-1]:
        for entry in pieces:
            start(entry)
    get_disp.wait()
    get_fix.wait()
    lax.fori_loop(1, layers, free_layer, 0)
    for comp in range(3):
        for i in range(layers):
            col_s[comp, i : i + 1, :] = moved[comp, i, 0:1, :]
    start(send_col)
    for entry in dens_copies[1:]:
        start(entry)

    @pl.when(r == nr - 1)
    def _():
        for comp in range(3):
            moved[comp, layers, plane, :] = jnp.zeros((rows, depth), jnp.float32)
            extra[comp, 1, plane, :] = jnp.zeros((rows, depth), jnp.float32)

    @pl.when(c == nc - 1)
    def _():
        col_r[...] = jnp.zeros_like(col_r)

    @pl.when(jnp.logical_not(there(1, 1)))
    def _():
        cor_r[...] = jnp.zeros_like(cor_r)
        cor_x[...] = jnp.zeros_like(cor_x)

    blank = jnp.zeros((8, depth), jnp.float32)
    for ref in (dens, sens):

        @pl.when(c == 0)
        def _():
            for i in range(half + 4):
                ref[i, low, :] = blank

        @pl.when(c == nc - 1)
        def _():
            for i in range(half + 4):
                ref[i, high, :] = blank

        @pl.when(jnp.logical_not(there(-dz, 0)))
        def _():
            for i in range(2):
                ref[lz + i] = jnp.zeros((rows + 16, depth), jnp.float32)

    arrive(send_col)
    for comp in range(3):
        for i in range(layers):
            moved[comp, i, pl.ds(rows, 1), :] = col_r[comp, i : i + 1, :]

    send_own = between(
        23, moved.at[:, layers - 1], extra.at[:, 0], 0, 0, 0, 1
    )
    start(send_own)

    ratio_sum = ratio[0]
    for case in range(1, ratio.shape[0]):
        ratio_sum = ratio_sum + ratio[case]
    total = jnp.full((8, depth), ratio_sum.astype(jnp.float32))
    share = jnp.full((8, depth), ratio[h].astype(jnp.float32)) / total
    share_x = jnp.full((8, depth), ratio[1 - h].astype(jnp.float32)) / total

    def energy_layers(first, count):
        def tile(j, _):
            row = pl.multiple_of(j * SHORT, SHORT)
            lower = node_modes(moved, first, row)
            for k in range(count):
                upper = node_modes(moved, first + k + 1, row)
                energy[first + k, pl.ds(row, SHORT), :] = share * energy_tile(lower, upper)
                lower = upper
            return 0

        lax.fori_loop(0, rows // SHORT, tile, 0)

    give = half * (1 - h)
    swap_a = remote(
        8, energy.at[pl.ds(give, half - 1)], other.at[pl.ds(0, half - 1)], 0, 0, 1 - h
    )
    swap_b = between(
        9, energy.at[pl.ds(half - 1, 1)], other.at[pl.ds(half - 1, 1)], 0, 0, 1, 0
    )
    energy_layers(give, half - 1)
    start(swap_a)
    energy_layers((half - 1) * h, half)
    start(swap_b)

    close, wide = 2 * (1 - h), 2 * h

    def scale_two(j):
        def tile(k, _):
            row = pl.multiple_of(k * TALL, TALL)
            cones = cone_tiles(dens, j, row, 2)
            for n in range(2):
                weights = weight_tile(
                    r * layers + half * h + j + n, nr * layers, c * rows + row, nc * rows, depth
                )
                inverse = 1.0 / weights
                physical = cones[n] * inverse
                alive = (1 - dead[j + n, pl.ds(row, TALL), :]).astype(jnp.float32)
                scale[j + n, pl.ds(row, TALL), :] = (
                    alive * (-3.0 * (1.0 - 0.001)) * physical * physical * inverse
                )
            return 0

        lax.fori_loop(0, rows // TALL, tile, 0)

    def sense(j):
        sens[2 + j, mid, :] = scale[j] * (energy[half * h + j] + other[j])

    get_dens.wait()
    get_dead.wait()
    arrive(dens_copies[1])
    arrive(dens_copies[2])
    scale_two(close)
    arrive(swap_a)
    arrive(swap_b)
    sense(close)
    sense(close + 1)

    ps, pd = pl.ds(half - (half - 2) * h, 2), pl.ds((half + 2) * h, 2)
    zs, zd = pl.ds(2 + (half - 2) * h, 2), pl.ds((half + 2) * (1 - h), 2)
    last, first = pl.ds(rows, 8), pl.ds(8, 8)
    close_copies = [
        remote(10, sens.at[ps, mid, :], sens.at[pd, mid, :], 0, 0, 1 - h),
        remote(12, sens.at[ps, last, :], sens.at[ps, low, :], 0, 1, h),
        remote(13, sens.at[ps, first, :], sens.at[ps, high, :], 0, -1, h),
        remote(14, sens.at[ps, last, :], sens.at[pd, low, :], 0, 1, 1 - h),
        remote(15, sens.at[ps, first, :], sens.at[pd, high, :], 0, -1, 1 - h),
    ]
    for entry in close_copies:
        start(entry)

    for n in (0, 3, 4):
        arrive(dens_copies[n])
    scale_two(wide)
    sense(wide)
    below = between(11, sens.at[pl.ds(2, 2), mid, :], sens.at[pl.ds(half + 2, 2), mid, :], -1, 0, 0, 1)
    above = between(22, sens.at[half, mid, :], sens.at[0, mid, :], 1, 0, 1, 0)
    last_layer = [
        between(
            32 + q,
            sens.at[half + 1, pl.ds(8 + q * tall, tall), :],
            sens.at[1, pl.ds(8 + q * tall, tall), :],
            1, 0, 1, 0,
        )
        for q in range(CHUNKS)
    ]
    start(above)

    @pl.when(h == 0)
    def _():
        sense(1)

    start(below)

    @pl.when(h == 1)
    def _():
        for entry in [*send_cor, send_own]:
            arrive(entry)
        for comp in range(3):
            moved[comp, layers, pl.ds(rows, 1), :] = cor_r[comp : comp + 1, :]
            extra[comp, 1, pl.ds(rows, 1), :] = cor_x[comp : comp + 1, :]
        for q in reversed(range(CHUNKS)):
            for entry in first_layer[q]:
                arrive(entry)

            def tile(k, _):
                row = pl.multiple_of(q * tall + k * SHORT, SHORT)
                here = pl.ds(row, SHORT)
                own = energy_tile(
                    node_modes(moved, layers - 1, row), node_modes(moved, layers, row)
                )
                his = energy_tile(node_modes(extra, 0, row), node_modes(extra, 1, row))
                sens[half + 1, pl.ds(row + 8, SHORT), :] = scale[half - 1, here, :] * (
                    share * own + share_x * his
                )
                return 0

            lax.fori_loop(0, tall // SHORT, tile, 0)
            start(last_layer[q])

    def flipped(index, src, dst, step_y):
        copy, goes, _ = remote(index, src, dst, -dz, step_y, 1 - h)
        return copy, goes, there(-dz, -step_y)

    wide_copies = [
        flipped(16, sens.at[zs, last, :], sens.at[zd, low, :], 1),
        flipped(17, sens.at[zs, first, :], sens.at[zd, high, :], -1),
    ]
    row_copies = [
        remote(18, sens.at[zs, last, :], sens.at[zs, low, :], 0, 1, h),
        remote(19, sens.at[zs, first, :], sens.at[zs, high, :], 0, -1, h),
    ]
    for entry in wide_copies + row_copies:
        start(entry)
    wide_copies = [below, above, *last_layer, *wide_copies]

    def filter_two(j):
        def tile(k, _):
            row = pl.multiple_of(k * TALL, TALL)
            cones = cone_tiles(sens, j, row, 2)
            for n in range(2):
                alive = (1 - dead[j + n, pl.ds(row, TALL), :]).astype(jnp.float32)
                out[half * h + j + n, pl.ds(row, TALL), :] = alive * cones[n]
            return 0

        lax.fori_loop(0, rows // TALL, tile, 0)

    def hand_over(index, j):
        place = pl.ds(half * h + j, 2)
        return remote(index, out.at[place], out.at[place], 0, 0, 1 - h)

    for entry in close_copies + row_copies:
        arrive(entry)
    filter_two(close)
    give_close, give_wide = hand_over(20, close), hand_over(21, wide)
    start(give_close)
    for entry in wide_copies:
        arrive(entry)
    filter_two(wide)
    start(give_wide)
    sent = [*dens_copies, send_col, *send_cor, swap_a, swap_b, send_own]
    for pieces in first_layer:
        sent.extend(pieces)
    for entry in sent + close_copies + wide_copies + row_copies + [give_close, give_wide]:
        left(entry)
    arrive(give_close)
    arrive(give_wide)


def shards(density, void_mask, fixed_mask, displacement, load_ratio):
    layers, rows, depth = density.shape
    half = layers // 2
    f32 = jnp.float32
    hbm = pl.BlockSpec(memory_space=pl.ANY)
    return pl.pallas_call(
        kernel,
        out_shape=pltpu.VMEM(density.shape, f32),
        in_specs=[pl.BlockSpec(memory_space=pltpu.SMEM), hbm, hbm, hbm, hbm],
        out_specs=pl.BlockSpec(memory_space=pltpu.VMEM),
        scratch_shapes=[
            pltpu.VMEM((3, layers + 1, rows + 8, depth), f32),
            pltpu.VMEM((3, 2, rows + 8, depth), f32),
            pltpu.VMEM((layers, rows, depth), jnp.int32),
            pltpu.VMEM((3, layers, depth), f32),
            pltpu.VMEM((3, layers, depth), f32),
            pltpu.VMEM((8, depth), f32),
            pltpu.VMEM((8, depth), f32),
            pltpu.VMEM((8, depth), f32),
            pltpu.VMEM((half + 4, rows + 16, depth), f32),
            pltpu.VMEM((half, rows, depth), jnp.int32),
            pltpu.VMEM((half, rows, depth), f32),
            pltpu.VMEM((layers, rows, depth), f32),
            pltpu.VMEM((half, rows, depth), f32),
            pltpu.VMEM((half + 4, rows + 16, depth), f32),
            pltpu.SemaphoreType.DMA((6,)),
            pltpu.SemaphoreType.DMA((N_COPIES,)),
            pltpu.SemaphoreType.DMA((N_COPIES,)),
        ],
        compiler_params=pltpu.CompilerParams(collective_id=0, has_side_effects=True),
    )(load_ratio, density, void_mask, fixed_mask, displacement)


def solution(mesh):
    placed = (
        P(("parts", "gz"), "gy", None),
        P(("parts", "gz"), "gy", None),
        P(("parts", "gz"), "gy", None),
        P("lc", None, ("parts", "gz"), "gy", None),
        P("parts"),
    )
    return jax.shard_map(
        shards,
        mesh=mesh,
        in_specs=placed,
        out_specs=P(("parts", "gz"), "gy", None),
        check_vma=False,
    )
```

```python
import math

import jax
import jax.numpy as jnp
from jax import lax
from jax.experimental import pallas as pl
from jax.experimental.pallas import tpu as pltpu
from jax.sharding import PartitionSpec as P

MESH = pl.DeviceIdType.MESH
POISSON = 0.3
FACTOR = 1.0 / ((1.0 + POISSON) * (1.0 - 2.0 * POISSON))
LAMBDA = POISSON * FACTOR
SHEAR = (0.5 - POISSON) * FACTOR
W = [2.5 - math.sqrt(d) for d in range(7)]
N_COPIES = 40
CHUNKS = 2
TALL = 32
SHORT = 8


def layer_classes(q0, q1, q2, q4, q5):
    p0 = W[0] * q0 + W[1] * q1 + W[2] * q2 + W[4] * q4 + W[5] * q5
    p1 = W[1] * q0 + W[2] * q1 + W[3] * q2 + W[5] * q4 + W[6] * q5
    p2 = W[4] * q0 + W[5] * q1 + W[6] * q2
    return p0, p1, p2


def lane_index(shape):
    return lax.broadcasted_iota(jnp.int32, shape, len(shape) - 1)


def lane_pair(field, step):
    depth = field.shape[-1]
    lane = lane_index(field.shape)
    after = jnp.where(lane < depth - step, pltpu.roll(field, depth - step, 1), 0.0)
    before = jnp.where(lane >= step, pltpu.roll(field, step, 1), 0.0)
    return after + before


def cone_tiles(ref, layer, row, count):
    window = TALL + 16
    f = [ref[layer + k, pl.ds(row, window), :] for k in range(count + 4)]
    mid = slice(8, 8 + TALL)

    def pair(t, step):
        return (pltpu.roll(t, step, 0) + pltpu.roll(t, window - step, 0))[mid]

    result = []
    for k in range(count):
        x0, x1, x2 = f[k + 2], f[k + 1] + f[k + 3], f[k] + f[k + 4]
        q0 = x0[mid]
        q1 = x1[mid] + pair(x0, 1)
        q2 = pair(x1, 1)
        q4 = x2[mid] + pair(x0, 2)
        q5 = pair(x2, 1) + pair(x1, 2)
        p0, p1, p2 = layer_classes(q0, q1, q2, q4, q5)
        result.append(p0 + lane_pair(p1, 1) + lane_pair(p2, 2))
    return result


def present(position, total, step):
    before = (position >= step).astype(jnp.float32)
    return before + (position + step < total).astype(jnp.float32)


def weight_tile(layer, layers, row, rows, depth):
    shape = (TALL, depth)
    sub = lax.broadcasted_iota(jnp.int32, shape, 0) + row
    spot = jnp.full(shape, layer, jnp.int32)
    nx1, nx2 = present(spot, layers, 1), present(spot, layers, 2)
    ny1, ny2 = present(sub, rows, 1), present(sub, rows, 2)
    one = jnp.ones(shape, jnp.float32)
    p0, p1, p2 = layer_classes(one, nx1 + ny1, nx1 * ny1, nx2 + ny2, nx2 * ny1 + nx1 * ny2)
    lane = lane_index(shape)
    return p0 + present(lane, depth, 1) * p1 + present(lane, depth, 2) * p2


def node_modes(ref, layer, row):
    result = []
    for comp in range(3):
        t = ref[comp, layer, pl.ds(row, SHORT + 8), :]
        depth, window = t.shape[-1], t.shape[0]
        tn = jnp.where(lane_index(t.shape) < depth - 1, pltpu.roll(t, depth - 1, 1), 0.0)
        s, d = t + tn, tn - t
        s0, d0 = s[0:SHORT], d[0:SHORT]
        s1, d1 = pltpu.roll(s, window - 1, 0)[0:SHORT], pltpu.roll(d, window - 1, 0)[0:SHORT]
        result.append((s0 + s1, d0 + d1, s1 - s0, d1 - d0))
    return result


def energy_tile(lower, upper):
    modes = []
    for a, b in zip(lower, upper):
        modes.append(
            {
                "x": b[0] - a[0],
                "z": a[1] + b[1],
                "y": a[2] + b[2],
                "yz": a[3] + b[3],
                "xz": b[1] - a[1],
                "xy": b[2] - a[2],
                "xyz": b[3] - a[3],
            }
        )
    u, v, w = modes
    sq = lambda t: t * t
    trace = sq(u["x"] + v["y"] + w["z"])
    linear = sq(v["xy"] + w["xz"]) + sq(u["xy"] + w["yz"]) + sq(u["xz"] + v["yz"])
    normal = sq(u["x"]) + sq(v["y"]) + sq(w["z"])
    bend = sq(u["xy"]) + sq(u["xz"]) + sq(v["xy"]) + sq(v["yz"]) + sq(w["yz"]) + sq(w["xz"])
    shear = sq(u["y"] + v["x"]) + sq(u["z"] + w["x"]) + sq(v["z"] + w["y"])
    twist = sq(u["yz"] + v["xz"]) + sq(u["yz"] + w["xy"]) + sq(v["xz"] + w["xy"])
    cubic = sq(u["xyz"]) + sq(v["xyz"]) + sq(w["xyz"])
    return (1.0 / 16.0) * (
        LAMBDA * trace
        + (LAMBDA / 3.0) * linear
        + (2.0 * SHEAR) * normal
        + SHEAR * (bend + shear)
        + (SHEAR / 3.0) * twist
        + ((LAMBDA + 4.0 * SHEAR) / 9.0) * cubic
    )


def kernel(
    ratio, density, void, fixed, disp, out,
    moved, extra, fix, col_s, col_r, cor_s, cor_r, cor_x, dens, dead, scale, energy, other, sens,
    local, send, recv,
):
    layers, rows, depth = density.shape
    half = layers // 2
    r, c, h = lax.axis_index("gz"), lax.axis_index("gy"), lax.axis_index("lc")
    nr, nc = lax.axis_size("gz"), lax.axis_size("gy")
    dz = 1 - 2 * h
    mid = pl.ds(8, rows)
    low, high = pl.ds(0, 8), pl.ds(rows + 8, 8)

    def there(step_z, step_y):
        z, y = r + step_z, c + step_y
        return (z >= 0) & (z < nr) & (y >= 0) & (y < nc)

    def remote(index, src, dst, step_z, step_y, core):
        copy = pltpu.make_async_remote_copy(
            src_ref=src, dst_ref=dst, send_sem=send.at[index], recv_sem=recv.at[index],
            device_id={"gz": r + step_z, "gy": c + step_y, "lc": core}, device_id_type=MESH,
        )
        goes, comes = there(step_z, step_y), there(-step_z, -step_y)
        return copy, goes, comes

    def between(index, src, dst, step_z, step_y, giver, taker):
        copy, goes, comes = remote(index, src, dst, step_z, step_y, taker)
        return copy, goes & (h == giver), comes & (h == taker)

    def start(entry):
        copy, goes, _ = entry
        pl.when(goes)(copy.start)

    def arrive(entry):
        copy, _, comes = entry
        pl.when(comes)(copy.wait_recv)

    def left(entry):
        copy, goes, _ = entry
        pl.when(goes)(copy.wait_send)

    l0, b0 = half // 2 * (1 - h), half // 2 * h
    keep = half + 2
    lz, sb = (half + 2) * h, (layers - 2) * (1 - h)
    plane, others = pl.ds(0, rows), pl.ds(1, layers - 1)
    get_disp0 = pltpu.make_async_copy(disp.at[0, :, 0], moved.at[:, 0, plane, :], local.at[0])
    get_fix0 = pltpu.make_async_copy(fixed.at[0], fix.at[0], local.at[1])
    get_disp = pltpu.make_async_copy(
        disp.at[0, :, others], moved.at[:, others, plane, :], local.at[2]
    )
    get_fix = pltpu.make_async_copy(fixed.at[others], fix.at[others], local.at[3])
    get_dens = pltpu.make_async_copy(
        density.at[pl.ds(b0, keep)], dens.at[pl.ds(l0, keep), mid, :], local.at[4]
    )
    get_dead = pltpu.make_async_copy(void.at[pl.ds(half * h, half)], dead, local.at[5])
    for copy in (get_disp0, get_fix0, get_disp, get_fix, get_dens, get_dead):
        copy.start()

    barrier = pltpu.get_barrier_semaphore()
    for step_z in (-1, 0, 1):
        for step_y in (-1, 0, 1):
            for flip in (0, 1):
                if step_z == 0 and step_y == 0 and flip == 0:
                    continue
                core = h if flip == 0 else 1 - h

                @pl.when(there(step_z, step_y))
                def _():
                    pl.semaphore_signal(
                        barrier, inc=1,
                        device_id={"gz": r + step_z, "gy": c + step_y, "lc": core},
                        device_id_type=MESH,
                    )

    span_z = 1 + (r > 0).astype(jnp.int32) + (r < nr - 1).astype(jnp.int32)
    span_y = 1 + (c > 0).astype(jnp.int32) + (c < nc - 1).astype(jnp.int32)

    own, edge = pl.ds(b0, keep), pl.ds(sb, 2)
    top, bottom = pl.ds(rows - 8, 8), pl.ds(0, 8)
    near, far = pl.ds(l0, keep), pl.ds(lz, 2)
    dens_copies = [
        remote(0, density.at[edge], dens.at[far, mid, :], dz, 0, h),
        remote(1, density.at[own, top, :], dens.at[near, low, :], 0, 1, h),
        remote(2, density.at[own, bottom, :], dens.at[near, high, :], 0, -1, h),
        remote(3, density.at[edge, top, :], dens.at[far, low, :], dz, 1, h),
        remote(4, density.at[edge, bottom, :], dens.at[far, high, :], dz, -1, h),
    ]

    def free_layer(i, _):
        free = (1 - fix[i]).astype(jnp.float32)
        for comp in range(3):
            moved[comp, i, plane, :] = moved[comp, i, plane, :] * free
        return 0

    tall = rows // CHUNKS
    chunks = [pl.ds(q * tall, tall) for q in range(CHUNKS)]
    first_layer = [
        [
            between(24 + q, moved.at[:, 0, part, :], extra.at[:, 1, part, :], -1, 0, 0, 1),
            between(28 + q, moved.at[:, 0, part, :], moved.at[:, layers, part, :], -1, 0, 1, 1),
        ]
        for q, part in enumerate(chunks)
    ]
    send_col = remote(6, col_s, col_r, 0, -1, h)
    send_cor = [
        between(7, cor_s, cor_r, -1, -1, 1, 1),
        between(5, cor_s, cor_x, -1, -1, 0, 1),
    ]
    get_disp0.wait()
    get_fix0.wait()
    free_layer(0, 0)
    for comp in range(3):
        cor_s[comp : comp + 1, :] = moved[comp, 0, 0:1, :]
    pl.semaphore_wait(barrier, 2 * span_z * span_y - 1)
    for entry in [*send_cor, *first_layer[-1]]:
        start(entry)
    for pieces in first_layer[-2::-1]:
        for entry in pieces:
            start(entry)
    get_disp.wait()
    get_fix.wait()
    lax.fori_loop(1, layers, free_layer, 0)
    for comp in range(3):
        for i in range(layers):
            col_s[comp, i : i + 1, :] = moved[comp, i, 0:1, :]
    start(send_col)
    for entry in dens_copies:
        start(entry)

    @pl.when(r == nr - 1)
    def _():
        for comp in range(3):
            moved[comp, layers, plane, :] = jnp.zeros((rows, depth), jnp.float32)
            extra[comp, 1, plane, :] = jnp.zeros((rows, depth), jnp.float32)

    @pl.when(c == nc - 1)
    def _():
        col_r[...] = jnp.zeros_like(col_r)

    @pl.when(jnp.logical_not(there(1, 1)))
    def _():
        cor_r[...] = jnp.zeros_like(cor_r)
        cor_x[...] = jnp.zeros_like(cor_x)

    blank = jnp.zeros((8, depth), jnp.float32)
    for ref in (dens, sens):

        @pl.when(c == 0)
        def _():
            for i in range(half + 4):
                ref[i, low, :] = blank

        @pl.when(c == nc - 1)
        def _():
            for i in range(half + 4):
                ref[i, high, :] = blank

        @pl.when(jnp.logical_not(there(-dz, 0)))
        def _():
            for i in range(2):
                ref[lz + i] = jnp.zeros((rows + 16, depth), jnp.float32)

    arrive(send_col)
    for comp in range(3):
        for i in range(layers):
            moved[comp, i, pl.ds(rows, 1), :] = col_r[comp, i : i + 1, :]

    send_own = between(
        23, moved.at[:, layers - 1], extra.at[:, 0], 0, 0, 0, 1
    )
    start(send_own)

    ratio_sum = ratio[0]
    for case in range(1, ratio.shape[0]):
        ratio_sum = ratio_sum + ratio[case]
    total = jnp.full((8, depth), ratio_sum.astype(jnp.float32))
    share = jnp.full((8, depth), ratio[h].astype(jnp.float32)) / total
    share_x = jnp.full((8, depth), ratio[1 - h].astype(jnp.float32)) / total

    def energy_layers(first, count):
        def tile(j, _):
            row = pl.multiple_of(j * SHORT, SHORT)
            lower = node_modes(moved, first, row)
            for k in range(count):
                upper = node_modes(moved, first + k + 1, row)
                energy[first + k, pl.ds(row, SHORT), :] = share * energy_tile(lower, upper)
                lower = upper
            return 0

        lax.fori_loop(0, rows // SHORT, tile, 0)

    give = half * (1 - h)
    swap_a = remote(
        8, energy.at[pl.ds(give, half - 1)], other.at[pl.ds(0, half - 1)], 0, 0, 1 - h
    )
    swap_b = between(
        9, energy.at[pl.ds(half - 1, 1)], other.at[pl.ds(half - 1, 1)], 0, 0, 1, 0
    )
    energy_layers(give, half - 1)
    start(swap_a)
    energy_layers((half - 1) * h, half)
    start(swap_b)

    close, wide = 2 * (1 - h), 2 * h

    def scale_two(j):
        def tile(k, _):
            row = pl.multiple_of(k * TALL, TALL)
            cones = cone_tiles(dens, j, row, 2)
            for n in range(2):
                weights = weight_tile(
                    r * layers + half * h + j + n, nr * layers, c * rows + row, nc * rows, depth
                )
                inverse = 1.0 / weights
                physical = cones[n] * inverse
                alive = (1 - dead[j + n, pl.ds(row, TALL), :]).astype(jnp.float32)
                scale[j + n, pl.ds(row, TALL), :] = (
                    alive * (-3.0 * (1.0 - 0.001)) * physical * physical * inverse
                )
            return 0

        lax.fori_loop(0, rows // TALL, tile, 0)

    def sense(j):
        sens[2 + j, mid, :] = scale[j] * (energy[half * h + j] + other[j])

    get_dens.wait()
    get_dead.wait()
    arrive(dens_copies[1])
    arrive(dens_copies[2])
    scale_two(close)
    arrive(swap_a)
    arrive(swap_b)
    sense(close)
    sense(close + 1)

    ps, pd = pl.ds(half - (half - 2) * h, 2), pl.ds((half + 2) * h, 2)
    zs, zd = pl.ds(2 + (half - 2) * h, 2), pl.ds((half + 2) * (1 - h), 2)
    last, first = pl.ds(rows, 8), pl.ds(8, 8)
    close_copies = [
        remote(10, sens.at[ps, mid, :], sens.at[pd, mid, :], 0, 0, 1 - h),
        remote(12, sens.at[ps, last, :], sens.at[ps, low, :], 0, 1, h),
        remote(13, sens.at[ps, first, :], sens.at[ps, high, :], 0, -1, h),
        remote(14, sens.at[ps, last, :], sens.at[pd, low, :], 0, 1, 1 - h),
        remote(15, sens.at[ps, first, :], sens.at[pd, high, :], 0, -1, 1 - h),
    ]
    for entry in close_copies:
        start(entry)

    for n in (0, 3, 4):
        arrive(dens_copies[n])
    scale_two(wide)
    sense(wide)
    below = between(11, sens.at[pl.ds(2, 2), mid, :], sens.at[pl.ds(half + 2, 2), mid, :], -1, 0, 0, 1)
    above = between(22, sens.at[half, mid, :], sens.at[0, mid, :], 1, 0, 1, 0)
    last_layer = [
        between(
            32 + q,
            sens.at[half + 1, pl.ds(8 + q * tall, tall), :],
            sens.at[1, pl.ds(8 + q * tall, tall), :],
            1, 0, 1, 0,
        )
        for q in range(CHUNKS)
    ]
    start(above)

    @pl.when(h == 0)
    def _():
        sense(1)

    start(below)

    @pl.when(h == 1)
    def _():
        for entry in [*send_cor, send_own]:
            arrive(entry)
        for comp in range(3):
            moved[comp, layers, pl.ds(rows, 1), :] = cor_r[comp : comp + 1, :]
            extra[comp, 1, pl.ds(rows, 1), :] = cor_x[comp : comp + 1, :]
        for q in reversed(range(CHUNKS)):
            for entry in first_layer[q]:
                arrive(entry)

            def tile(k, _):
                row = pl.multiple_of(q * tall + k * SHORT, SHORT)
                here = pl.ds(row, SHORT)
                own = energy_tile(
                    node_modes(moved, layers - 1, row), node_modes(moved, layers, row)
                )
                his = energy_tile(node_modes(extra, 0, row), node_modes(extra, 1, row))
                sens[half + 1, pl.ds(row + 8, SHORT), :] = scale[half - 1, here, :] * (
                    share * own + share_x * his
                )
                return 0

            lax.fori_loop(0, tall // SHORT, tile, 0)
            start(last_layer[q])

    def flipped(index, src, dst, step_y):
        copy, goes, _ = remote(index, src, dst, -dz, step_y, 1 - h)
        return copy, goes, there(-dz, -step_y)

    wide_copies = [
        flipped(16, sens.at[zs, last, :], sens.at[zd, low, :], 1),
        flipped(17, sens.at[zs, first, :], sens.at[zd, high, :], -1),
    ]
    row_copies = [
        remote(18, sens.at[zs, last, :], sens.at[zs, low, :], 0, 1, h),
        remote(19, sens.at[zs, first, :], sens.at[zs, high, :], 0, -1, h),
    ]
    for entry in wide_copies + row_copies:
        start(entry)
    wide_copies = [below, above, *last_layer, *wide_copies]

    def filter_two(j):
        def tile(k, _):
            row = pl.multiple_of(k * TALL, TALL)
            cones = cone_tiles(sens, j, row, 2)
            for n in range(2):
                alive = (1 - dead[j + n, pl.ds(row, TALL), :]).astype(jnp.float32)
                out[half * h + j + n, pl.ds(row, TALL), :] = alive * cones[n]
            return 0

        lax.fori_loop(0, rows // TALL, tile, 0)

    def hand_over(index, j):
        place = pl.ds(half * h + j, 2)
        return remote(index, out.at[place], out.at[place], 0, 0, 1 - h)

    for entry in close_copies + row_copies:
        arrive(entry)
    filter_two(close)
    give_close, give_wide = hand_over(20, close), hand_over(21, wide)
    start(give_close)
    for entry in wide_copies:
        arrive(entry)
    filter_two(wide)
    start(give_wide)
    sent = [*dens_copies, send_col, *send_cor, swap_a, swap_b, send_own]
    for pieces in first_layer:
        sent.extend(pieces)
    for entry in sent + close_copies + wide_copies + row_copies + [give_close, give_wide]:
        left(entry)
    arrive(give_close)
    arrive(give_wide)


def shards(density, void_mask, fixed_mask, displacement, load_ratio):
    layers, rows, depth = density.shape
    half = layers // 2
    f32 = jnp.float32
    hbm = pl.BlockSpec(memory_space=pl.ANY)
    return pl.pallas_call(
        kernel,
        out_shape=pltpu.VMEM(density.shape, f32),
        in_specs=[pl.BlockSpec(memory_space=pltpu.SMEM), hbm, hbm, hbm, hbm],
        out_specs=pl.BlockSpec(memory_space=pltpu.VMEM),
        scratch_shapes=[
            pltpu.VMEM((3, layers + 1, rows + 8, depth), f32),
            pltpu.VMEM((3, 2, rows + 8, depth), f32),
            pltpu.VMEM((layers, rows, depth), jnp.int32),
            pltpu.VMEM((3, layers, depth), f32),
            pltpu.VMEM((3, layers, depth), f32),
            pltpu.VMEM((8, depth), f32),
            pltpu.VMEM((8, depth), f32),
            pltpu.VMEM((8, depth), f32),
            pltpu.VMEM((half + 4, rows + 16, depth), f32),
            pltpu.VMEM((half, rows, depth), jnp.int32),
            pltpu.VMEM((half, rows, depth), f32),
            pltpu.VMEM((layers, rows, depth), f32),
            pltpu.VMEM((half, rows, depth), f32),
            pltpu.VMEM((half + 4, rows + 16, depth), f32),
            pltpu.SemaphoreType.DMA((6,)),
            pltpu.SemaphoreType.DMA((N_COPIES,)),
            pltpu.SemaphoreType.DMA((N_COPIES,)),
        ],
        compiler_params=pltpu.CompilerParams(collective_id=0, has_side_effects=True),
    )(load_ratio, density, void_mask, fixed_mask, displacement)


def solution(mesh):
    placed = (
        P(("parts", "gz"), "gy", None),
        P(("parts", "gz"), "gy", None),
        P(("parts", "gz"), "gy", None),
        P("lc", None, ("parts", "gz"), "gy", None),
        P("parts"),
    )
    return jax.shard_map(
        shards,
        mesh=mesh,
        in_specs=placed,
        out_specs=P(("parts", "gz"), "gy", None),
        check_vma=False,
    )
```
